512 devices in a mesh: box: 16 (over z), row: 4 (over y_hi, core), col: 8 (over x, y_lo).
Axes of the slice: x: 4, y: 4 (y_hi: 2, y_lo: 2; y = y_hi * 2 + y_lo), z: 16, core: 2. Of those that a mesh axis runs over, the one named last changes fastest.
Arguments:
- ext_ext: float32 [16, 3072, 3072], P('box', 'row', 'col'), may hold values from -6 to 6
- ext_int: float32 [16, 3072, 1024], P('box', 'row', 'col'), may hold values from -0.1875 to 0.1875
- int_ext: float32 [16, 1024, 3072], P('box', 'row', 'col'), may hold values from -6 to 6
- int_int: float32 [16, 1024, 1024], P('box', 'row', 'col'), may hold values from -0.1 to 0.1, as said below
Outputs:
- merged: float32 [16, 3072, 2, 3072], P('box', 'row', None, 'col')
The draws below stay inside these ranges and needn't reach their ends.
Inputs may be any that keep to these rules, and one draw needn't show every extreme that they name: `int_int`: independent entries.
All inputs are finite; a program needn't handle non-finite values.
Results may differ from the reference program's by a relative error of at most 0.0003.
Values sent between devices are 32-bit elements; how exact they have to be, the bound alone decides.
A program may use at most 64 MiB of HBM per device.

```python
import jax
import jax.numpy as jnp
from jax import lax

NE = 3072
NI = 1024
BOXES = 16


def draw_int_int(key, part):
    scale = 0.8 / NI ** 0.5
    values = jnp.clip(jax.random.normal(key, (BOXES, NI, NI), jnp.float32), -4.0, 4.0)
    return values * scale


def block_levels(stream_key, extent, split, smallest, largest):
    def one(dim, shards_of):
        draws = jax.random.uniform(jax.random.fold_in(jax.random.fold_in(stream_key, 6), dim), (shards_of,), jnp.float32, smallest / len(split), largest / len(split))
        return jnp.repeat(jnp.exp(draws), extent[dim] // shards_of).reshape((-1,) + (1,) * (len(extent) - dim - 1))

    loudness = one(*split[0])
    for cut in split[1:]:
        loudness = loudness * one(*cut)
    return loudness


def noise(stream_key, dims, spread, bound, pieces=(), held_as=jnp.bfloat16):
    drawn = jax.random.normal(stream_key, dims, jnp.float32) * spread
    if len(pieces) > 0:
        drawn = block_levels(stream_key, dims, pieces, -0.22, 0.18) * drawn
    return jnp.clip(drawn, min=-bound, max=bound).astype(held_as)


def setup_inputs(seed: int = 0) -> dict:
    key_list = jax.random.split(jax.random.key(seed), 5)
    ext_ext = noise(key_list[0], (BOXES, NE, NE), 1.0, 6.0, ((0, 16), (1, 4), (2, 8)), jnp.float32)
    ext_int = noise(key_list[1], (BOXES, NE, NI), NI ** -0.5, 0.1875, ((0, 16), (1, 4), (2, 8)), jnp.float32)
    int_ext = noise(key_list[2], (BOXES, NI, NE), 1.0, 6.0, ((0, 16), (1, 4), (2, 8)), jnp.float32)
    int_int = draw_int_int(jax.random.fold_in(key_list[4], 71), 0)
    return {"ext_ext": ext_ext, "ext_int": ext_int, "int_ext": int_ext, "int_int": int_int}


def merge_one(items):
    ee, ed, de, dd, partner_de, partner_dd, parity = items
    hi = lax.Precision.HIGHEST
    coupling = jnp.dot(partner_dd, dd, precision=hi, preferred_element_type=jnp.float32)
    square = jnp.dot(coupling, coupling, precision=hi, preferred_element_type=jnp.float32)
    first = jnp.eye(NI, dtype=coupling.dtype) + coupling
    inverse = first + jnp.dot(first, square, precision=hi, preferred_element_type=jnp.float32)
    coupled = jnp.dot(partner_dd, de, precision=hi, preferred_element_type=jnp.float32)
    is_even = parity == 0
    source_zero = jnp.where(is_even, coupled, partner_de)
    source_one = jnp.where(is_even, partner_de, coupled)
    carried_zero = jnp.dot(inverse, source_zero, precision=hi, preferred_element_type=jnp.float32)
    carried_one = jnp.dot(inverse, source_one, precision=hi, preferred_element_type=jnp.float32)
    zeros = jnp.zeros_like(ee)
    merged_zero = jnp.where(is_even, ee, zeros) + jnp.dot(ed, carried_zero, precision=hi, preferred_element_type=jnp.float32)
    merged_one = jnp.where(is_even, zeros, ee) + jnp.dot(ed, carried_one, precision=hi, preferred_element_type=jnp.float32)
    return jnp.stack([merged_zero, merged_one], axis=1)


def swapped(array):
    shape = array.shape
    return array.reshape((BOXES // 2, 2) + shape[1:])[:, ::-1].reshape(shape)


def reference(ext_ext, ext_int, int_ext, int_int):
    parity = (jnp.arange(BOXES) % 2).astype(jnp.int32)
    items = (ext_ext, ext_int, int_ext, int_int, swapped(int_ext), swapped(int_int), parity)
    return lax.map(merge_one, items)
```

```python
import jax
import jax.numpy as jnp
from jax import lax
from jax.experimental import pallas as pl
from jax.experimental.pallas import tpu as pltpu
from jax.sharding import PartitionSpec as P

MESH = pl.DeviceIdType.MESH
F32 = jnp.float32
BF16 = jnp.bfloat16
SIDE = 4
MAX_COPIES = 160


def merge_kernel(ni, rows, cols, width, out_rows, dd_ref, de_ref, ed_ref, out_ref,
                 own_dd, partner_dd, de_parts, de_relay, de_other, ed, carr,
                 dd_hi, dd_lo, pd_hi, pd_lo, ed_hi, ed_lo, source, cat_a, cat_b,
                 send_sem, recv_sem, local_sem):
    box = lax.axis_index("box")
    row = lax.axis_index("row")
    col = lax.axis_index("col")
    core = row % 2
    x = col // 2
    y = row // 2 * 2 + col % 2
    other_box = box + 1 - 2 * (box % 2)
    yh = row // 2

    def near(dx=0, dy=0):
        there_x = (x + dx + SIDE) % SIDE
        there_y = (y + dy + SIDE) % SIDE
        return (box, there_y // 2 * 2 + core, there_x * 2 + there_y % 2)

    sibling = (box, yh * 2 + 1 - core, col)
    across = (other_box, row, col)
    y_pair = (box, row, x * 2 + 1 - col % 2)
    peers = [near(1), near(-1), near(0, 1), near(0, -1), across, sibling]

    made = [0]
    sent = []

    def send(src, dst, device):
        n = made[0]
        made[0] += 1
        copy = pltpu.make_async_remote_copy(
            src_ref=src, dst_ref=dst, send_sem=send_sem.at[n], recv_sem=recv_sem.at[n],
            device_id=device, device_id_type=MESH)
        copy.start()
        sent.append(copy)
        return n

    def arrived(n, ref, device):
        pltpu.make_async_remote_copy(
            src_ref=ref, dst_ref=ref, send_sem=send_sem.at[n], recv_sem=recv_sem.at[n],
            device_id=device, device_id_type=MESH).wait_recv()

    def block(buf, dx=0, dy=0, half=None, who=None):
        there_x = (x + dx + SIDE) % SIDE
        there_y = (y + dy + SIDE) % SIDE
        held_by = core if who is None else who
        start = (there_y // 2 * 2 + held_by) * rows
        size = rows
        if half is not None:
            size = rows // 2
            start = start + half * size
        return buf.at[there_x * 2 + there_y % 2, pl.ds(pl.multiple_of(start, 8), size), :]

    class Ring:
        def __init__(self, part, step):
            self.part = part
            self.step = step

        def first(self):
            own = self.part(0, None)
            self.up = send(own, own, self.step(1))
            self.down = send(own, own, self.step(-1))

        def second(self):
            arrived(self.up, self.part(-1, None), self.step(-1))
            low = self.part(-1, 0)
            self.up2 = send(low, low, self.step(1))
            arrived(self.down, self.part(1, None), self.step(1))
            high = self.part(1, 1)
            self.down2 = send(high, high, self.step(-1))

        def third(self):
            arrived(self.up2, self.part(2, 0), self.step(-1))
            arrived(self.down2, self.part(2, 1), self.step(1))

    def ring_x(buf, dy):
        return Ring(lambda d, half: block(buf, d, dy, half), lambda d: near(d))

    def ring_y(buf, dx):
        return Ring(lambda d, half: block(buf, dx, d, half), lambda d: near(0, d))

    shared = []

    def share(buf, dx, dy):
        mine = block(buf, dx, dy)
        shared.append((send(mine, mine, sibling), block(buf, dx, dy, None, 1 - core)))

    barrier = pltpu.get_barrier_semaphore()
    for peer in peers:
        pl.semaphore_signal(barrier, inc=1, device_id=peer, device_id_type=MESH)
    load_dd = pltpu.make_async_copy(dd_ref, block(own_dd), local_sem.at[0])
    load_de = pltpu.make_async_copy(de_ref, de_parts.at[0, yh], local_sem.at[1])
    load_ed = pltpu.make_async_copy(ed_ref, ed.at[col], local_sem.at[2])
    load_dd.start()
    load_de.start()
    load_ed.start()
    load_dd.wait()
    pl.semaphore_wait(barrier, len(peers))

    half_rows = rows // 2
    top = pl.ds(0, half_rows)
    bottom = pl.ds(half_rows, half_rows)

    z_dd = send(block(own_dd), block(partner_dd), across)
    px = ring_x(own_dd, 0)
    px.first()
    load_de.wait()
    de_up = send(de_parts.at[0, yh, top], de_relay.at[0], near(0, 1))
    de_down = send(de_parts.at[0, yh, bottom], de_relay.at[1], near(0, -1))
    z_de = send(de_parts.at[0, yh], de_parts.at[1, yh], across)
    py = {0: ring_y(own_dd, 0)}
    py[0].first()
    share(own_dd, 0, 0)
    load_ed.wait()

    arrived(z_dd, block(partner_dd), across)
    qy = ring_y(partner_dd, 0)
    qy.first()
    qx = {0: ring_x(partner_dd, 0)}
    qx[0].first()
    share(partner_dd, 0, 0)

    px.second()
    for d in (-1, 1):
        py[d] = ring_y(own_dd, d)
        py[d].first()
        share(own_dd, d, 0)
    from_below = (y - 1 + SIDE) % SIDE // 2
    from_above = (y + 1) % SIDE // 2
    arrived(de_up, de_relay.at[0], near(0, -1))
    de_up2 = send(de_relay.at[0], de_parts.at[0, from_below, top], near(0, 1))
    arrived(de_down, de_relay.at[1], near(0, 1))
    de_down2 = send(de_relay.at[1], de_parts.at[0, from_above, bottom], near(0, -1))

    qy.second()
    for d in (-1, 1):
        qx[d] = ring_x(partner_dd, d)
        qx[d].first()
        share(partner_dd, 0, d)

    ed_half = out_rows // 2
    ed_quarter = out_rows // 4

    def ed_part(flip, base):
        def part(d, half):
            there = (x + d + SIDE) % SIDE * 2 + (1 - col % 2 if flip else col % 2)
            if half is None:
                return ed.at[there, pl.ds(base, ed_half), :]
            return ed.at[there, pl.ds(base + half * ed_quarter, ed_quarter), :]
        return Ring(part, lambda d: near(d))

    ex = ed_part(False, ed_half)
    ex.first()

    py[0].second()
    qx[0].second()
    share(own_dd, 0, -1)
    share(own_dd, 0, 1)
    share(partner_dd, -1, 0)
    share(partner_dd, 1, 0)

    px.third()
    py[2] = ring_y(own_dd, 2)
    py[2].first()
    share(own_dd, 2, 0)
    qy.third()
    qx[2] = ring_x(partner_dd, 2)
    qx[2].first()
    share(partner_dd, 0, 2)

    arrived(de_up2, de_parts.at[0, 1 - yh, top], near(0, -1))
    arrived(de_down2, de_parts.at[0, 1 - yh, bottom], near(0, 1))
    z_de2 = send(de_parts.at[0, 1 - yh], de_parts.at[1, 1 - yh], across)

    for d in (-1, 1):
        py[d].second()
        qx[d].second()
        share(own_dd, d, -1)
        share(own_dd, d, 1)
        share(partner_dd, -1, d)
        share(partner_dd, 1, d)
    own_ed_up = ed.at[col, pl.ds(0, ed_half), :]
    e_pair = send(own_ed_up, own_ed_up, y_pair)
    ex.second()
    eo = ed_part(False, 0)
    eo.first()

    py[0].third()
    share(own_dd, 0, 2)
    qx[0].third()
    share(partner_dd, 2, 0)

    py[2].second()
    qx[2].second()
    share(own_dd, 2, -1)
    share(own_dd, 2, 1)
    share(partner_dd, -1, 2)
    share(partner_dd, 1, 2)
    for d in (-1, 1):
        py[d].third()
        qx[d].third()
        share(own_dd, d, 2)
        share(partner_dd, 2, d)
    arrived(z_de, de_parts.at[1, yh], across)
    arrived(z_de2, de_parts.at[1, 1 - yh], across)
    de_share = [send(de_parts.at[1 - core, h], de_other.at[h], sibling) for h in range(2)]

    py[2].third()
    qx[2].third()
    share(own_dd, 2, 2)
    share(partner_dd, 2, 2)
    for n, ref in shared:
        arrived(n, ref, sibling)
    for h in range(2):
        arrived(de_share[h], de_other.at[h], sibling)

    def split(value):
        high = value.astype(BF16)
        return high, (value - high.astype(F32)).astype(BF16)

    tile = 256
    blocks = ni // cols

    def split_all(buf, hi, lo, count):
        step = 128

        def body(i, carry):
            at = pl.ds(pl.multiple_of(i * step, step), step)
            for c in range(blocks):
                h, l = split(buf[c, at, :])
                hi[at, c * cols:(c + 1) * cols] = h
                lo[at, c * cols:(c + 1) * cols] = l
            return carry

        lax.fori_loop(0, count // step, body, 0)

    def put(cat, at, value):
        h, l = split(value)
        cat[at, :width] = h
        cat[at, width:] = l

    split_all(own_dd, dd_hi, dd_lo, ni)
    split_all(partner_dd, pd_hi, pd_lo, ni)

    for h in range(2):
        for who in range(2):
            at = pl.ds((h * 2 + who) * rows, rows)
            value = jnp.where(core == who, de_parts[core, h], de_other[h])
            source[at, :] = value
            put(cat_a, at, value)

    def product(hi, lo, cat, done, count=ni):
        def body(i, carry):
            at = pl.ds(pl.multiple_of(i * tile, tile), tile)
            both = jnp.dot(hi[at, :], cat[...], preferred_element_type=F32)
            cross = jnp.dot(lo[at, :], cat[:, :width], preferred_element_type=F32)
            done(at, both[:, :width] + (both[:, width:] + cross))
            return carry

        lax.fori_loop(0, count // tile, body, 0)

    def to_source(at, value):
        source[at, :] = value
        put(cat_b, at, value)

    def to_source_sum(at, value):
        value = source[at, :] + value
        source[at, :] = value
        put(cat_b, at, value)

    def to_a(at, value):
        put(cat_a, at, value)

    def to_b(at, value):
        put(cat_b, at, value)

    def to_carried(at, value):
        carr[core, at, :] = source[at, :] + value

    @pl.when(core == 0)
    def _():
        product(pd_hi, pd_lo, cat_a, to_source)

    @pl.when(core == 1)
    def _():
        cat_b[...] = cat_a[...]

    product(dd_hi, dd_lo, cat_b, to_a)
    ex.third()
    arrived(e_pair, ed.at[x * 2 + 1 - col % 2, pl.ds(0, ed_half), :], y_pair)
    ep = ed_part(True, 0)
    ep.first()
    eo.second()

    def low_rows(d, flip):
        there = (x + d + SIDE) % SIDE * 2 + (1 - col % 2 if flip else col % 2)
        return ed.at[there, pl.ds(ed_half, ed_half), :]

    e_last = [(send(low_rows(d, False), low_rows(d, False), y_pair), low_rows(d, True))
              for d in (0, 1, -1, 2)]
    product(pd_hi, pd_lo, cat_a, to_b)
    eo.third()
    ep.second()
    product(dd_hi, dd_lo, cat_b, to_a)
    product(pd_hi, pd_lo, cat_a, to_source_sum)
    product(dd_hi, dd_lo, cat_b, to_a)
    ep.third()
    for n, ref in e_last:
        arrived(n, ref, y_pair)
    product(pd_hi, pd_lo, cat_a, to_carried)
    mine = send(carr.at[core], carr.at[core], sibling)

    split_all(ed, ed_hi, ed_lo, out_rows)

    def fill(kind):
        def body(i, carry):
            at = pl.ds(pl.multiple_of(i * 128, 128), 128)
            put(cat_b, at, carr[kind, at, :])
            return carry

        lax.fori_loop(0, ni // 128, body, 0)

    def final(kind):
        slot = (kind + box) % 2

        def done(at, value):
            out_ref[slot, at, :] = value

        fill(kind)
        product(ed_hi, ed_lo, cat_b, done, out_rows)

    final(core)
    arrived(mine, carr.at[1 - core], sibling)
    final(1 - core)

    for copy in sent:
        copy.wait_send()


def local(ext_ext, ext_int, int_ext, int_int):
    dd, de, ed, ee = int_int[0], int_ext[0], ext_int[0], ext_ext[0]
    rows, cols = dd.shape
    width = de.shape[1]
    out_rows = ed.shape[0]
    ni = rows * lax.axis_size("row")
    blocks = ni // cols

    def body(*refs):
        merge_kernel(ni, rows, cols, width, out_rows, *refs)

    product = pl.pallas_call(
        body,
        out_shape=jax.ShapeDtypeStruct((2, out_rows, width), F32),
        in_specs=[pl.BlockSpec(memory_space=pl.ANY)] * 3,
        out_specs=pl.BlockSpec(memory_space=pltpu.VMEM),
        scratch_shapes=[
            pltpu.VMEM((blocks, ni, cols), F32),
            pltpu.VMEM((blocks, ni, cols), F32),
            pltpu.VMEM((2, 2, rows, width), F32),
            pltpu.VMEM((2, rows // 2, width), F32),
            pltpu.VMEM((2, rows, width), F32),
            pltpu.VMEM((blocks, out_rows, cols), F32),
            pltpu.VMEM((2, ni, width), F32),
            pltpu.VMEM((ni, ni), BF16),
            pltpu.VMEM((ni, ni), BF16),
            pltpu.VMEM((ni, ni), BF16),
            pltpu.VMEM((ni, ni), BF16),
            pltpu.VMEM((out_rows, ni), BF16),
            pltpu.VMEM((out_rows, ni), BF16),
            pltpu.VMEM((ni, width), F32),
            pltpu.VMEM((ni, 2 * width), BF16),
            pltpu.VMEM((ni, 2 * width), BF16),
            pltpu.SemaphoreType.DMA((MAX_COPIES,)),
            pltpu.SemaphoreType.DMA((MAX_COPIES,)),
            pltpu.SemaphoreType.DMA((3,)),
        ],
        compiler_params=pltpu.CompilerParams(
            collective_id=0, has_side_effects=True, vmem_limit_bytes=60 * 2**20),
    )(dd, de, ed)
    slot = lax.broadcasted_iota(jnp.int32, (1, 2, 1), 1)
    keep = slot == lax.axis_index("box") % 2
    merged = jnp.where(keep, ee[:, None, :], 0.0) + jnp.swapaxes(product, 0, 1)
    return merged[None]


def solution(mesh):
    placed = P("box", "row", "col")
    return jax.shard_map(
        local, mesh=mesh, in_specs=(placed,) * 4, out_specs=P("box", "row", None, "col"),
        check_vma=False)
```

```python
import jax
import jax.numpy as jnp
from jax import lax
from jax.experimental import pallas as pl
from jax.experimental.pallas import tpu as pltpu
from jax.sharding import PartitionSpec as P

MESH = pl.DeviceIdType.MESH
F32 = jnp.float32
BF16 = jnp.bfloat16
SIDE = 4
MAX_COPIES = 224
RELAY_AT = (2, 2, 4, 5, 6, 12, 12)
ED_UP = 352


def merge_kernel(ni, rows, cols, width, out_rows, dd_ref, de_ref, ed_ref, ee_ref, out_ref,
                 own_dd, partner_dd, de_parts, de_other, ed, carr,
                 dd_hi, dd_lo, pd_hi, pd_lo, ed_hi, ed_lo, source, cat_a, cat_b, ee,
                 send_sem, recv_sem, local_sem):
    box = lax.axis_index("box")
    row = lax.axis_index("row")
    col = lax.axis_index("col")
    core = row % 2
    x = col // 2
    y = row // 2 * 2 + col % 2
    other_box = box + 1 - 2 * (box % 2)
    yh = row // 2

    def near(dx=0, dy=0):
        there_x = (x + dx + SIDE) % SIDE
        there_y = (y + dy + SIDE) % SIDE
        return (box, there_y // 2 * 2 + core, there_x * 2 + there_y % 2)

    sibling = (box, yh * 2 + 1 - core, col)
    across = (other_box, row, col)
    y_pair = (box, row, x * 2 + 1 - col % 2)
    far_x, far_y = near(2), near(0, 2)
    peers = [near(1), near(-1), near(0, 1), near(0, -1), far_x, far_y, across, sibling]

    made = [0]
    sent = []

    def send(src, dst, device):
        n = made[0]
        made[0] += 1
        copy = pltpu.make_async_remote_copy(
            src_ref=src, dst_ref=dst, send_sem=send_sem.at[n], recv_sem=recv_sem.at[n],
            device_id=device, device_id_type=MESH)
        copy.start()
        sent.append(copy)
        return n

    def arrived(n, ref, device):
        pltpu.make_async_remote_copy(
            src_ref=ref, dst_ref=ref, send_sem=send_sem.at[n], recv_sem=recv_sem.at[n],
            device_id=device, device_id_type=MESH).wait_recv()

    def block(buf, dx=0, dy=0, piece=(0, 1), who=None):
        there_x = (x + dx + SIDE) % SIDE
        there_y = (y + dy + SIDE) % SIDE
        held_by = core if who is None else who
        at, of = piece
        size = rows // of
        start = (there_y // 2 * 2 + held_by) * rows + at * size
        return buf.at[there_x * 2 + there_y % 2, pl.ds(pl.multiple_of(start, 8), size), :]

    class Ring:
        def __init__(self, part, step):
            self.part = part
            self.step = step

        def first(self):
            own = self.part(0, None)
            self.up = send(own, own, self.step(1))
            self.down = send(own, own, self.step(-1))

        def second(self):
            arrived(self.up, self.part(-1, None), self.step(-1))
            low = self.part(-1, 0)
            self.up2 = send(low, low, self.step(1))
            arrived(self.down, self.part(1, None), self.step(1))
            high = self.part(1, 1)
            self.down2 = send(high, high, self.step(-1))

        def third(self):
            arrived(self.up2, self.part(2, 0), self.step(-1))
            arrived(self.down2, self.part(2, 1), self.step(1))

    class Direct:
        def __init__(self, part, step):
            self.part = part
            self.step = step

        def first(self):
            own = self.part(0)
            self.sent = {d: send(own, own, self.step(d)) for d in (1, -1, 2)}

        def second(self):
            for d in (1, -1):
                arrived(self.sent[d], self.part(-d), self.step(-d))

        def third(self):
            arrived(self.sent[2], self.part(2), self.step(2))

    def direct_x(buf, piece=(0, 1)):
        return Direct(lambda d: block(buf, d, 0, piece), lambda d: near(d))

    def direct_y(buf, piece=(0, 1)):
        return Direct(lambda d: block(buf, 0, d, piece), lambda d: near(0, d))

    def ring_x(buf, dy, piece=(0, 1)):
        at, of = piece

        def part(d, half):
            if half is None:
                return block(buf, d, dy, piece)
            return block(buf, d, dy, (at * 2 + half, of * 2))

        return Ring(part, near)

    def ring_y(buf, dx, piece=(0, 1)):
        at, of = piece

        def part(d, half):
            if half is None:
                return block(buf, dx, d, piece)
            return block(buf, dx, d, (at * 2 + half, of * 2))

        return Ring(part, lambda d: near(0, d))

    shared = {}

    def share(buf, dx, dy):
        mine = block(buf, dx, dy)
        whose = shared.setdefault(id(buf), [])
        whose.append((send(mine, mine, sibling), block(buf, dx, dy, who=1 - core)))

    def shares_arrived(buf):
        for n, ref in shared[id(buf)]:
            arrived(n, ref, sibling)

    def split(value):
        high = value.astype(BF16)
        return high, (value - high.astype(F32)).astype(BF16)

    tile = 256
    blocks = ni // cols

    def split_all(buf, hi, lo, count):
        step = 128

        def body(i, carry):
            at = pl.ds(pl.multiple_of(i * step, step), step)
            for c in range(blocks):
                h, l = split(buf[c, at, :])
                hi[at, c * cols:(c + 1) * cols] = h
                lo[at, c * cols:(c + 1) * cols] = l
            return carry

        lax.fori_loop(0, count // step, body, 0)

    def put(cat, at, value):
        h, l = split(value)
        cat[at, :width] = h
        cat[at, width:] = l

    barrier = pltpu.get_barrier_semaphore()
    for peer in peers:
        pl.semaphore_signal(barrier, inc=1, device_id=peer, device_id_type=MESH)
    load_dd = pltpu.make_async_copy(dd_ref, block(own_dd), local_sem.at[0])
    load_de = pltpu.make_async_copy(de_ref, de_parts.at[0, yh], local_sem.at[1])
    load_ed = pltpu.make_async_copy(ed_ref, ed.at[col], local_sem.at[2])
    load_dd.start()
    load_de.start()
    load_ed.start()
    load_ee = pltpu.make_async_copy(ee_ref, ee, local_sem.at[3])
    load_ee.start()
    load_dd.wait()
    pl.semaphore_wait(barrier, len(peers))

    TOP, BOTTOM = (0, 2), (1, 2)

    def ed_ring(flip, base, size):
        def part(d, half):
            there = (x + d + SIDE) % SIDE * 2 + (1 - col % 2 if flip else col % 2)
            if half is None:
                return ed.at[there, pl.ds(base, size), :]
            return ed.at[there, pl.ds(base + half * (size // 2), size // 2), :]
        return Ring(part, near)

    ed_up = ED_UP
    ed_low = out_rows - ed_up
    z_dd = send(block(own_dd), block(partner_dd), across)
    px = direct_x(own_dd, TOP)
    px.first()
    oy = direct_y(own_dd, BOTTOM)
    oy.first()
    ox = {0: ring_x(own_dd, 0, BOTTOM)}
    ox[0].first()
    py = {0: ring_y(own_dd, 0, TOP)}
    py[0].first()
    load_de.wait()
    z_de = send(de_parts.at[0, yh], de_parts.at[1, yh], across)
    share(own_dd, 0, 0)
    load_ed.wait()
    load_ee.wait()

    def to_py(d):
        py[d] = ring_y(own_dd, d, TOP)
        py[d].first()

    def to_ox(d):
        ox[d] = ring_x(own_dd, d, BOTTOM)
        ox[d].first()

    arrived(z_dd, block(partner_dd), across)
    qy = direct_y(partner_dd)
    qy.first()
    own = block(partner_dd)
    qx_up = send(own, own, near(1))
    qx_down = send(own, own, near(-1))
    share(partner_dd, 0, 0)

    px.second()
    to_py(-1)
    to_py(1)
    oy.second()
    to_ox(-1)
    to_ox(1)
    px.third()
    to_py(2)
    oy.third()
    to_ox(2)
    y_de = send(de_parts.at[0, yh], de_parts.at[0, yh], far_y)

    ox[0].second()
    for d in (-1, 1):
        share(own_dd, d, 0)
    py[0].second()
    for d in (-1, 1):
        share(own_dd, 0, d)

    qx = {}

    def to_qx(d):
        qx[d] = ring_x(partner_dd, d)
        qx[d].first()
        share(partner_dd, 0, d)

    qy.second()
    to_qx(-1)
    to_qx(1)
    qy.third()
    to_qx(2)
    ox[0].third()
    z_row = send(block(own_dd, 2, 0), block(partner_dd, 2, 0), across)
    share(own_dd, 2, 0)
    arrived(qx_up, block(partner_dd, -1, 0), near(-1))
    share(partner_dd, -1, 0)
    arrived(qx_down, block(partner_dd, 1, 0), near(1))
    share(partner_dd, 1, 0)

    for d in (-1, 1):
        py[d].second()
        ox[d].second()
    py[0].third()
    share(own_dd, 0, 2)
    py[2].second()
    ox[2].second()
    arrived(y_de, de_parts.at[0, 1 - yh], far_y)
    z_de2 = send(de_parts.at[0, 1 - yh], de_parts.at[1, 1 - yh], across)


    for d in (-1, 1):
        qx[d].second()
        for e in (-1, 1):
            share(partner_dd, e, d)
    for d in (-1, 1):
        for e in (-1, 1):
            share(own_dd, d, e)
    qx[2].second()
    for e in (-1, 1):
        share(partner_dd, e, 2)
    own_ed_up = ed.at[col, pl.ds(0, ed_up), :]
    e_pair = send(own_ed_up, own_ed_up, y_pair)
    ex = ed_ring(False, ed_up, ed_low)
    ex.first()
    eo = ed_ring(False, 0, ed_up)
    eo.first()
    for d in (-1, 1):
        py[d].third()
        ox[d].third()
    for d in (-1, 1):
        share(own_dd, d, 2)
        share(own_dd, 2, d)
    py[2].third()
    ox[2].third()
    share(own_dd, 2, 2)
    shares_arrived(own_dd)
    split_all(own_dd, dd_hi, dd_lo, ni)
    for d in (-1, 1):
        qx[d].third()
        share(partner_dd, 2, d)
    arrived(z_row, block(partner_dd, 2, 0), across)
    share(partner_dd, 2, 0)
    arrived(z_de, de_parts.at[1, yh], across)
    arrived(z_de2, de_parts.at[1, 1 - yh], across)
    de_share = [send(de_parts.at[1 - core, h], de_other.at[h], sibling) for h in range(2)]
    qx[2].third()
    share(partner_dd, 2, 2)

    shares_arrived(partner_dd)
    split_all(partner_dd, pd_hi, pd_lo, ni)
    for h in range(2):
        arrived(de_share[h], de_other.at[h], sibling)

    for h in range(2):
        for who in range(2):
            at = pl.ds((h * 2 + who) * rows, rows)
            value = jnp.where(core == who, de_parts[core, h], de_other[h])
            source[at, :] = value
            put(cat_a, at, value)

    def product(hi, lo, cat, done, count=ni, first=0):
        def body(i, carry):
            at = pl.ds(pl.multiple_of(i * tile, tile), tile)
            both = jnp.dot(hi[at, :], cat[...], preferred_element_type=F32)
            cross = jnp.dot(lo[at, :], cat[:, :width], preferred_element_type=F32)
            done(at, both[:, :width] + (both[:, width:] + cross))
            return carry

        lax.fori_loop(first // tile, count // tile, body, 0)

    def to_source(at, value):
        source[at, :] = value
        put(cat_b, at, value)

    def to_source_sum(at, value):
        value = source[at, :] + value
        source[at, :] = value
        put(cat_b, at, value)

    def to_a(at, value):
        put(cat_a, at, value)

    def to_b(at, value):
        put(cat_b, at, value)

    def to_carried(at, value):
        value = source[at, :] + value
        carr[core, at, :] = value
        put(cat_b, at, value)

    @pl.when(core == 0)
    def _():
        product(pd_hi, pd_lo, cat_a, to_source)

    @pl.when(core == 1)
    def _():
        cat_b[...] = cat_a[...]

    e_last = []

    def low_rows(d, flip):
        there = (x + d + SIDE) % SIDE * 2 + (1 - col % 2 if flip else col % 2)
        return ed.at[there, pl.ds(ed_up, ed_low), :]

    def low_to_pair(d):
        e_last.append((send(low_rows(d, False), low_rows(d, False), y_pair), low_rows(d, True)))

    rings = {}

    def upper_of_pair():
        arrived(e_pair, ed.at[x * 2 + 1 - col % 2, pl.ds(0, ed_up), :], y_pair)
        rings["ep"] = ed_ring(True, 0, ed_up)
        rings["ep"].first()
        low_to_pair(0)

    def lower_second():
        ex.second()
        low_to_pair(1)
        low_to_pair(-1)

    def lower_third():
        ex.third()
        low_to_pair(2)

    steps = [upper_of_pair, lower_second, lambda: eo.second(), lower_third,
             lambda: rings["ep"].second(), lambda: eo.third(), lambda: rings["ep"].third()]
    chain = [(dd_hi, dd_lo, cat_b, to_a), (pd_hi, pd_lo, cat_a, to_b),
             (dd_hi, dd_lo, cat_b, to_a), (pd_hi, pd_lo, cat_a, to_source_sum),
             (dd_hi, dd_lo, cat_b, to_a), (pd_hi, pd_lo, cat_a, to_carried)]
    half = ni // 2

    def half_of(kind, n):
        return carr.at[kind, pl.ds(n * half, half), :]

    def send_half(n):
        return send(half_of(core, n), half_of(core, n), sibling)

    for n in range(2 * len(chain)):
        for step, when in zip(steps, RELAY_AT):
            if when == n:
                step()
        if n == 2 * len(chain) - 1:
            mine = [send_half(0)]
        product(*chain[n // 2], half * (n % 2 + 1), half * (n % 2))
    mine.append(send_half(1))
    for step, when in zip(steps, RELAY_AT):
        if when == 2 * len(chain):
            step()
    for n, ref in e_last:
        arrived(n, ref, y_pair)

    split_all(ed, ed_hi, ed_lo, out_rows)

    def fill(kind):
        def body(i, carry):
            at = pl.ds(pl.multiple_of(i * 128, 128), 128)
            put(cat_b, at, carr[kind, at, :])
            return carry

        lax.fori_loop(0, ni // 128, body, 0)

    def final(kind):
        slot = (kind + box) % 2

        def done(at, value):
            value = jnp.where(kind == 0, ee[at, :], 0.0) + value
            out_ref[slot, at, :] = value

        product(ed_hi, ed_lo, cat_b, done, out_rows)

    final(core)
    for n in range(2):
        arrived(mine[n], half_of(1 - core, n), sibling)
    fill(1 - core)
    final(1 - core)

    for copy in sent:
        copy.wait_send()


def local(ext_ext, ext_int, int_ext, int_int):
    dd, de, ed, ee = int_int[0], int_ext[0], ext_int[0], ext_ext[0]
    rows, cols = dd.shape
    width = de.shape[1]
    out_rows = ed.shape[0]
    ni = rows * lax.axis_size("row")
    blocks = ni // cols

    def body(*refs):
        merge_kernel(ni, rows, cols, width, out_rows, *refs)

    product = pl.pallas_call(
        body,
        out_shape=jax.ShapeDtypeStruct((2, out_rows, width), F32),
        in_specs=[pl.BlockSpec(memory_space=pl.ANY)] * 4,
        out_specs=pl.BlockSpec(memory_space=pltpu.VMEM),
        scratch_shapes=[
            pltpu.VMEM((blocks, ni, cols), F32),
            pltpu.VMEM((blocks, ni, cols), F32),
            pltpu.VMEM((2, 2, rows, width), F32),
            pltpu.VMEM((2, rows, width), F32),
            pltpu.VMEM((blocks, out_rows, cols), F32),
            pltpu.VMEM((2, ni, width), F32),
            pltpu.VMEM((ni, ni), BF16),
            pltpu.VMEM((ni, ni), BF16),
            pltpu.VMEM((ni, ni), BF16),
            pltpu.VMEM((ni, ni), BF16),
            pltpu.VMEM((out_rows, ni), BF16),
            pltpu.VMEM((out_rows, ni), BF16),
            pltpu.VMEM((ni, width), F32),
            pltpu.VMEM((ni, 2 * width), BF16),
            pltpu.VMEM((ni, 2 * width), BF16),
            pltpu.VMEM((out_rows, width), F32),
            pltpu.SemaphoreType.DMA((MAX_COPIES,)),
            pltpu.SemaphoreType.DMA((MAX_COPIES,)),
            pltpu.SemaphoreType.DMA((4,)),
        ],
        compiler_params=pltpu.CompilerParams(
            collective_id=0, has_side_effects=True, vmem_limit_bytes=60 * 2**20),
    )(dd, de, ed, ee)
    return jnp.swapaxes(product, 0, 1)[None]


def solution(mesh):
    placed = P("box", "row", "col")
    return jax.shard_map(
        local, mesh=mesh, in_specs=(placed,) * 4, out_specs=P("box", "row", None, "col"),
        check_vma=False)
```
